32 devices in a mesh: groups: 2 (over y), seq: 4 (over z), tp: 4 (over x, core).
Axes of the slice: x: 2, y: 2, z: 4, core: 2. Of those that a mesh axis runs over, the one named last changes fastest.
Arguments:
- resp_queries: bfloat16 [4096, 8192], P(('groups', 'seq'), 'tp'), parts along dimension 0, may hold values from -300 to 300
- resp_keys: bfloat16 [4096, 1024], P(('groups', 'seq'), 'tp'), parts along dimension 0, may hold values from -4 to 4
- resp_values: bfloat16 [4096, 1024], P(('groups', 'seq'), 'tp'), parts along dimension 0, may hold values from -48 to 48
- prompt_keys: bfloat16 [2048, 1024], P(('groups', 'seq'), 'tp'), parts along dimension 0, may hold values from -4 to 4
- prompt_values: bfloat16 [2048, 1024], P(('groups', 'seq'), 'tp'), parts along dimension 0, may hold values from -48 to 48
- out_weight: bfloat16 [8192, 8192], P('tp', 'seq'), may hold values from -0.0625 to 0.0625
- resp_blocks: int32 [8], P('groups'), parts along dimension 0, may hold values from 1 to 4, 11 in all
Outputs:
- attended: bfloat16 [4096, 8192], P(('groups', 'seq'), 'tp'), parts along dimension 0
The draws below stay inside these ranges and needn't reach their ends.
There are 2 independent parts, one for each index of `groups`. The reference program is written for one: setup_inputs(seed, part) draws one part's arguments, and reference() takes and returns one part's arrays. A program takes and returns all parts, laid end to end along the dimension named above; an argument that names none is the same for every part. Nothing has to cross between parts.
Inputs may be any that keep to these rules, and one draw needn't show every extreme that they name: `resp_blocks`: the lengths sum to 11 blocks and the longest is exactly 4 blocks.
All inputs are finite; a program needn't handle non-finite values.
Results may differ from the reference program's by a relative error of at most 0.017.
Values may be sent and summed in bfloat16 or wider, within the bound.
A program may use at most 128 MiB of HBM per device.

```python
import math
import jax
import jax.numpy as jnp
import numpy as np
from jax import lax

D = 8192
H = 64
KVH = 8
HD = 128
BLOCK = 128
MAXB = 4
PROMPT = 1024
NRESP = 4
TOTB = 11
N_TP = 4


def prompt_base(key):
    base = jax.random.normal(jax.random.fold_in(key, 11), (PROMPT, KVH * HD), jnp.float32)
    base = jnp.clip(base, -4.0, 4.0)
    return base


def draw_prompt_keys(key, part):
    return prompt_base(key).astype(jnp.bfloat16)


def draw_resp_queries(key, part):
    count = NRESP * MAXB * BLOCK
    values = 1.5 * jax.random.normal(jax.random.fold_in(key, 23), (count, H * HD), jnp.float32)
    values = jnp.clip(values, -9.0, 9.0)
    return values.astype(jnp.bfloat16)


def block_scale(rng, dims, split, smallest, top_value):
    loudness, own = 1.0, jax.random.fold_in(rng, 6)
    for dim, shards_of in split:
        heights = jnp.exp(jax.random.uniform(jax.random.fold_in(own, dim), (shards_of,), jnp.float32, smallest / len(split), top_value / len(split)))
        loudness = loudness * jnp.repeat(heights, dims[dim] // shards_of).reshape([-1 if axis == dim else 1 for axis in range(len(dims))])
    return loudness


def length_profile(amount, total, limit, lean):
    loads = [(1 << 20) // math.isqrt(standing ** lean) + 1 for standing in range(2, amount + 1)]
    rest, given = total - limit - (amount - 1), [1] * (amount - 1)
    while rest > 0:
        candidates = [i for i in range(amount - 1) if given[i] < limit]
        pool, left = sum([loads[i] for i in candidates]), rest
        for i in candidates:
            extra = min(limit - given[i], max(1, left * loads[i] // pool), rest)
            given[i] = given[i] + extra
            rest = rest - extra
    return np.array([limit] + given)


def ragged_sizes(rng, number_of, total, reach, skew):
    if number_of == 2:
        one = jax.random.randint(rng, (), max(1, total - reach), min(reach, total - 1) + 1)
        return jnp.stack([one, total - one])
    lengths = jnp.asarray(length_profile(number_of, total, reach, skew), jnp.int32)
    twos = (number_of - 1) // 2
    source_of, receiver = lengths[1:1 + 2 * twos:2], lengths[2:2 + 2 * twos:2]
    slack = jnp.minimum(source_of - 1, reach - receiver)
    shifted = jax.random.randint(jax.random.fold_in(rng, 1), (twos,), 0, 1 << 20) % (slack + 1)
    lengths = lengths.at[1:1 + 2 * twos:2].set(source_of - shifted).at[2:2 + 2 * twos:2].set(receiver + shifted)
    return lengths[jax.random.permutation(jax.random.fold_in(rng, 2), number_of)]


def bell_draw(rng, shape, scale, bound, split=(), kind=jnp.bfloat16):
    loudness = block_scale(rng, shape, split, -0.22, 0.18) if split else 1.0
    drawn = jax.random.normal(rng, shape, jnp.float32) * scale * loudness
    return jnp.minimum(jnp.maximum(drawn, -bound), bound).astype(kind)


def setup_inputs(seed: int = 0, part: int = 0) -> dict:
    seeds = jax.random.split(jax.random.key(seed), 8)
    own_keys = jax.random.split(jax.random.fold_in(seeds[7], part), 8)
    return {
        "resp_queries": draw_resp_queries(jax.random.fold_in(jax.random.fold_in(seeds[7], part), 71), part),
        "resp_keys": bell_draw(own_keys[1], (NRESP * MAXB * BLOCK, KVH * HD), 1.0, 4.0, ((0, 4), (1, 4))),
        "resp_values": bell_draw(own_keys[2], (NRESP * MAXB * BLOCK, KVH * HD), 8.0, 48.0, ((0, 4), (1, 4))),
        "prompt_keys": draw_prompt_keys(jax.random.fold_in(jax.random.fold_in(seeds[7], part), 71), part),
        "prompt_values": bell_draw(own_keys[4], (PROMPT, KVH * HD), 8.0, 48.0, ((0, 4), (1, 4))),
        "out_weight": bell_draw(seeds[5], (H * HD, D), (H * HD) ** -0.5, 0.0625, ((0, 4), (1, 4))),
        "resp_blocks": ragged_sizes(own_keys[6], NRESP, TOTB, MAXB, 1).astype(jnp.int32),
    }


def reference(resp_queries, resp_keys, resp_values, prompt_keys, prompt_values, out_weight, resp_blocks):
    span = MAXB * BLOCK
    group = H // KVH
    scale = HD ** -0.5
    width = H * HD // N_TP
    prompt_k = prompt_keys.astype(jnp.float32)
    prompt_v = prompt_values.astype(jnp.float32)

    def one_response(packed):
        queries, keys, values, blocks = packed
        length = blocks * BLOCK
        position = jnp.arange(span, dtype=jnp.int32)
        all_keys = jnp.concatenate([prompt_k, keys.astype(jnp.float32)], axis=0)
        all_values = jnp.concatenate([prompt_v, values.astype(jnp.float32)], axis=0)
        allowed = jnp.concatenate([jnp.ones((span, PROMPT), dtype=bool), position[None, :] <= position[:, None]], axis=1)
        pieces = []
        for head_group in range(KVH):
            query_part = queries[:, head_group * group * HD:(head_group + 1) * group * HD].astype(jnp.float32).reshape(span, group, HD)
            key_part = all_keys[:, head_group * HD:(head_group + 1) * HD]
            value_part = all_values[:, head_group * HD:(head_group + 1) * HD]
            scores = jnp.einsum('qhd,nd->hqn', query_part, key_part) * scale
            scores = jnp.where(allowed[None], scores, -jnp.inf)
            top = jnp.max(scores, axis=-1, keepdims=True)
            expo = jnp.exp(scores - top)
            total = jnp.sum(expo, axis=-1, keepdims=True)
            rounded = lax.optimization_barrier(expo.astype(jnp.bfloat16)).astype(jnp.float32)
            numer = jnp.einsum('hqn,nd->hqd', rounded, value_part)
            heads = (numer / total).astype(jnp.bfloat16)
            pieces.append(jnp.transpose(heads, (1, 0, 2)).reshape(span, group * HD))
        attn = jnp.concatenate(pieces, axis=1)
        summed = jnp.zeros((span, D), jnp.float32)
        for tensor_index in range(N_TP):
            partial_value = jnp.dot(attn[:, tensor_index * width:(tensor_index + 1) * width], out_weight[tensor_index * width:(tensor_index + 1) * width], preferred_element_type=jnp.float32)
            summed = summed + lax.optimization_barrier(partial_value.astype(jnp.bfloat16)).astype(jnp.float32)
        live = position < length
        return jnp.where(live[:, None], summed, jnp.zeros_like(summed)).astype(jnp.bfloat16)

    result = lax.map(one_response, (resp_queries.reshape(NRESP, span, H * HD), resp_keys.reshape(NRESP, span, KVH * HD), resp_values.reshape(NRESP, span, KVH * HD), resp_blocks))
    return result.reshape(NRESP * span, D)
```

```python
import functools
import jax
import jax.numpy as jnp
from jax import lax
from jax.experimental import pallas as pl
from jax.experimental.pallas import tpu as pltpu
from jax.sharding import PartitionSpec as P

HD = 128
BLOCK = 128
MAXB = 4
LOG2E = 1.4426950408889634


def attend_block(q, kp, vp, kr, vr, first, rows):
    c = (HD ** -0.5) * LOG2E
    nt = (((1,), (1,)), ((), ()))
    sp = lax.dot_general(q, kp, nt, preferred_element_type=jnp.float32)
    sr = lax.dot_general(q, kr, nt, preferred_element_type=jnp.float32)
    qpos = lax.broadcasted_iota(jnp.int32, sr.shape, 0) % rows + first
    kpos = lax.broadcasted_iota(jnp.int32, sr.shape, 1)
    sr = jnp.where(kpos <= qpos, sr, -1e30)
    m = jnp.maximum(
        jnp.max(sp, axis=1, keepdims=True), jnp.max(sr, axis=1, keepdims=True)
    )
    ep = jnp.exp2((sp - m) * c)
    er = jnp.exp2((sr - m) * c)
    total = jnp.sum(ep, axis=1, keepdims=True) + jnp.sum(er, axis=1, keepdims=True)
    acc = jnp.dot(ep.astype(jnp.bfloat16), vp, preferred_element_type=jnp.float32)
    acc = acc + jnp.dot(er.astype(jnp.bfloat16), vr, preferred_element_type=jnp.float32)
    return (acc / total).astype(jnp.bfloat16)


def attn_kernel(group, q_ref, kp_ref, vp_ref, kr_ref, vr_ref, o_ref):
    first = pl.program_id(1) * BLOCK
    half = max(group // 2, 1)
    for h in range(0, group, half):
        q = jnp.concatenate(
            [q_ref[:, (h + g) * HD : (h + g + 1) * HD] for g in range(half)], axis=0
        )
        o = attend_block(
            q, kp_ref[...], vp_ref[...], kr_ref[...], vr_ref[...], first, BLOCK
        )
        for g in range(half):
            o_ref[:, (h + g) * HD : (h + g + 1) * HD] = o[g * BLOCK : (g + 1) * BLOCK]


def attention(q, pkv, kr, vr):
    rows, head_cols = q.shape
    kv_local = kr.shape[1] // HD
    group = head_cols // kr.shape[1]
    prompt = pkv.shape[0]
    return pl.pallas_call(
        functools.partial(attn_kernel, group),
        grid=(kv_local, rows // BLOCK),
        out_shape=jax.ShapeDtypeStruct((rows, head_cols), jnp.bfloat16),
        in_specs=[
            pl.BlockSpec((BLOCK, group * HD), lambda k, b: (b, k)),
            pl.BlockSpec((prompt, HD), lambda k, b: (0, k)),
            pl.BlockSpec((prompt, HD), lambda k, b: (0, k + kv_local)),
            pl.BlockSpec((rows, HD), lambda k, b: (0, k)),
            pl.BlockSpec((rows, HD), lambda k, b: (0, k)),
        ],
        out_specs=pl.BlockSpec((BLOCK, group * HD), lambda k, b: (b, k)),
        compiler_params=pltpu.CompilerParams(vmem_limit_bytes=60000 * 1024),
    )(q, pkv, pkv, kr, vr)


def per_device(
    resp_queries, resp_keys, resp_values, prompt_keys, prompt_values, out_weight, resp_blocks
):
    nseq = lax.axis_size("seq")
    ntp = lax.axis_size("tp")
    rows = resp_queries.shape[0]
    assert rows == MAXB * BLOCK and nseq % ntp == 0
    count = resp_blocks.shape[0]
    slots = count + 3 * count // 4 + MAXB
    cols = out_weight.shape[1]

    pkv = lax.all_gather(
        jnp.concatenate([prompt_keys, prompt_values], axis=1), "seq", axis=0, tiled=True
    )
    heads = attention(resp_queries, pkv, resp_keys, resp_values)
    gathered = lax.all_gather(heads, "seq", axis=0, tiled=True)

    ends = jnp.cumsum(resp_blocks)
    starts = ends - resp_blocks
    slot = jnp.arange(slots, dtype=jnp.int32)
    owner = jnp.sum((ends[None, :] <= slot[:, None]).astype(jnp.int32), axis=1)
    source = owner * MAXB + slot - jnp.take(starts, owner)
    packed = jnp.take(gathered.reshape(count * MAXB, BLOCK, -1), source, axis=0)
    partial = jnp.dot(
        packed.reshape(slots * BLOCK, -1), out_weight, preferred_element_type=jnp.float32
    ).astype(jnp.bfloat16)
    piece = lax.psum_scatter(partial, "tp", scatter_dimension=1, tiled=True)
    width = piece.shape[1]
    offset = jnp.arange(MAXB, dtype=jnp.int32)
    where = jnp.minimum(starts[:, None] + offset[None, :], slots - 1).reshape(-1)
    alive = (offset[None, :] < resp_blocks[:, None]).reshape(-1)
    padded = jnp.take(piece.reshape(slots, BLOCK, width), where, axis=0)
    padded = jnp.where(alive[:, None, None], padded, jnp.zeros_like(padded))
    padded = padded.reshape(nseq, rows, width)
    owned = lax.all_to_all(padded, "seq", split_axis=0, concat_axis=0, tiled=True)
    mine = lax.all_to_all(owned, "tp", split_axis=0, concat_axis=0, tiled=True)
    mine = mine.reshape(ntp, nseq // ntp, rows, width).transpose(2, 1, 0, 3)
    return mine.reshape(rows, (nseq // ntp) * cols)


def solution(mesh):
    return jax.shard_map(
        per_device,
        mesh=mesh,
        in_specs=(
            P(("groups", "seq"), "tp"),
            P(("groups", "seq"), "tp"),
            P(("groups", "seq"), "tp"),
            P(("groups", "seq"), "tp"),
            P(("groups", "seq"), "tp"),
            P("tp", "seq"),
            P("groups"),
        ),
        out_specs=P(("groups", "seq"), "tp"),
        check_vma=False,
    )
```

```python
import functools
import jax
import jax.numpy as jnp
from jax import lax
from jax.experimental import pallas as pl
from jax.experimental.pallas import tpu as pltpu
from jax.sharding import PartitionSpec as P

HD = 128
BLOCK = 128
MAXB = 4
LOG2E = 1.4426950408889634


def attend_block(q, kp, vp, kr, vr, first, rows):
    c = (HD ** -0.5) * LOG2E
    nt = (((1,), (1,)), ((), ()))
    sp = lax.dot_general(q, kp, nt, preferred_element_type=jnp.float32)
    sr = lax.dot_general(q, kr, nt, preferred_element_type=jnp.float32)
    qpos = lax.broadcasted_iota(jnp.int32, sr.shape, 0) % rows + first
    kpos = lax.broadcasted_iota(jnp.int32, sr.shape, 1)
    sr = jnp.where(kpos <= qpos, sr, -1e30)
    m = jnp.maximum(
        jnp.max(sp, axis=1, keepdims=True), jnp.max(sr, axis=1, keepdims=True)
    )
    ep = jnp.exp2((sp - m) * c)
    er = jnp.exp2((sr - m) * c)
    total = jnp.sum(ep, axis=1, keepdims=True) + jnp.sum(er, axis=1, keepdims=True)
    acc = jnp.dot(ep.astype(jnp.bfloat16), vp, preferred_element_type=jnp.float32)
    acc = acc + jnp.dot(er.astype(jnp.bfloat16), vr, preferred_element_type=jnp.float32)
    return (acc / total).astype(jnp.bfloat16)


MESH = pl.DeviceIdType.MESH


def fused_kernel(
    nseq, ntp, group,
    lens_ref, q_ref, kr_ref, vr_ref, pkv_ref, w_ref, out_ref,
    prompt, gath, part, half_in, quart_in, final,
    p_send, p_recv, g_send, g_recv, a_send, a_recv, b_send, b_recv, f_send, f_recv,
):
    s = lax.axis_index("seq")
    t = lax.axis_index("tp")
    core, x = lax.rem(t, 2), lax.div(t, 2)
    partner = t + 1 - 2 * core
    nx = ntp // 2
    per = nseq // ntp
    chunks = nseq * MAXB
    prows = pkv_ref.shape[0]
    cols = w_ref.shape[1]
    half = BLOCK // 2
    quart = half // nx
    kv_local = kr_ref.shape[1] // HD
    has_right, has_left = s < nseq - 1, s > 0
    home = lax.div(s, per)
    slab = lax.rem(s, per)

    def p_copy(r, side):
        return pltpu.make_async_remote_copy(
            src_ref=prompt.at[pl.ds(r * prows, prows)],
            dst_ref=prompt.at[pl.ds(r * prows, prows)],
            send_sem=p_send.at[side, r],
            recv_sem=p_recv.at[r],
            device_id={"seq": s - 1 + 2 * side},
            device_id_type=MESH,
        )

    def g_copy(r, b, side):
        return pltpu.make_async_remote_copy(
            src_ref=gath.at[r, b],
            dst_ref=gath.at[r, b],
            send_sem=g_send.at[side, r, b],
            recv_sem=g_recv.at[r, b],
            device_id={"seq": s - 1 + 2 * side},
            device_id_type=MESH,
        )

    def a_copy(i):
        return pltpu.make_async_remote_copy(
            src_ref=part.at[i, pl.ds((1 - core) * half, half)],
            dst_ref=half_in.at[i],
            send_sem=a_send.at[i],
            recv_sem=a_recv.at[i],
            device_id={"tp": partner},
            device_id_type=MESH,
        )

    def b_copy(i, k):
        other = lax.rem(x + k, nx)
        return pltpu.make_async_remote_copy(
            src_ref=part.at[i, pl.ds(core * half + other * quart, quart)],
            dst_ref=quart_in.at[i, k - 1],
            send_sem=b_send.at[i, k - 1],
            recv_sem=b_recv.at[i, k - 1],
            device_id={"tp": other * 2 + core},
            device_id_type=MESH,
        )

    def f_copy(i, r, b):
        return pltpu.make_async_remote_copy(
            src_ref=final.at[i],
            dst_ref=out_ref.at[slab, pl.ds(b * BLOCK + core * half + x * quart, quart)],
            send_sem=f_send.at[i],
            recv_sem=f_recv.at[b, slab, t],
            device_id={"seq": r, "tp": home},
            device_id_type=MESH,
        )

    both = jnp.minimum(s, nseq - 1 - s)
    far_side = jnp.where(s > nseq - 1 - s, -1, 1)

    def chunk_of(i):
        j = jnp.maximum(i - MAXB, 0)
        twin = 2 * MAXB
        jj = jnp.maximum(j - twin * both, 0)
        near = j < twin * both
        d = jnp.where(near, lax.div(j, twin) + 1, both + 1 + lax.div(jj, MAXB))
        b = jnp.where(near, lax.div(lax.rem(j, twin), 2), lax.rem(jj, MAXB))
        side = jnp.where(near, 2 * lax.rem(j, 2) - 1, far_side)
        own = i < MAXB
        return jnp.where(own, s, s + side * d), jnp.where(own, i, b)

    def loop(n, fn, start=0):
        def step(i, carry):
            fn(i)
            return carry

        lax.fori_loop(start, n, step, 0)

    prompt[pl.ds(s * prows, prows), :] = pkv_ref[...]

    @pl.when(has_left)
    def _():
        p_copy(s, 0).start()

    @pl.when(has_right)
    def _():
        p_copy(s, 1).start()

    def gather_prompt(d):
        @pl.when(s - d >= 0)
        def _():
            p_copy(s - d, 1).wait_recv()

            @pl.when(has_right)
            def _():
                p_copy(s - d, 1).start()

        @pl.when(s + d < nseq)
        def _():
            p_copy(s + d, 0).wait_recv()

            @pl.when(has_left)
            def _():
                p_copy(s + d, 0).start()

    loop(nseq, gather_prompt, 1)

    def stage_a(i):
        r, b = chunk_of(i)

        @pl.when(i < MAXB)
        def _():
            first = i * BLOCK
            run = max(group // 2, 1)
            for k in range(kv_local):
                kcol = slice(k * HD, (k + 1) * HD)
                vcol = slice((kv_local + k) * HD, (kv_local + k + 1) * HD)
                for h in range(k * group, (k + 1) * group, run):
                    q = jnp.concatenate(
                        [
                            q_ref[pl.ds(first, BLOCK), (h + g) * HD : (h + g + 1) * HD]
                            for g in range(run)
                        ],
                        axis=0,
                    )
                    o = attend_block(
                        q, prompt[:, kcol], prompt[:, vcol], kr_ref[:, kcol], vr_ref[:, kcol],
                        first, BLOCK,
                    )
                    for g in range(run):
                        gath[s, i, :, (h + g) * HD : (h + g + 1) * HD] = o[
                            g * BLOCK : (g + 1) * BLOCK
                        ]

        @pl.when(i >= MAXB)
        def _():
            g_copy(r, b, 0).wait_recv()

        @pl.when(has_right & (r <= s))
        def _():
            g_copy(r, b, 1).start()

        @pl.when(has_left & (r >= s))
        def _():
            g_copy(r, b, 0).start()

        part[i] = jnp.dot(
            gath[r, b], w_ref[...], preferred_element_type=jnp.float32
        ).astype(jnp.bfloat16)
        a_copy(i).start()

    def stage_b(i):
        a_copy(i).wait_recv()
        mine = pl.ds(core * half, half)
        part[i, mine, :] = (
            part[i, mine, :].astype(jnp.float32) + half_in[i].astype(jnp.float32)
        ).astype(jnp.bfloat16)
        for k in range(1, nx):
            b_copy(i, k).start()

    def stage_c(i):
        r, b = chunk_of(i)
        for k in range(1, nx):
            b_copy(i, k).wait_recv()
        total = part[i, pl.ds(core * half + x * quart, quart), :].astype(jnp.float32)
        for k in range(1, nx):
            total = total + quart_in[i, k - 1].astype(jnp.float32)
        row = lax.broadcasted_iota(jnp.int32, total.shape, 0)
        row = row + (b * BLOCK + core * half + x * quart)
        total = jnp.where(row < lens_ref[r] * BLOCK, total, 0.0)
        final[i] = total.astype(jnp.bfloat16)
        here = (r == s) & (home == t)

        @pl.when(here)
        def _():
            out_ref[slab, pl.ds(b * BLOCK + core * half + x * quart, quart), :] = final[i]

        @pl.when(jnp.logical_not(here))
        def _():
            f_copy(i, r, b).start()

    def step(i):
        @pl.when(i < chunks)
        def _():
            stage_a(i)

        @pl.when((i >= 1) & (i < chunks + 1))
        def _():
            stage_b(i - 1)

        @pl.when(i >= 2)
        def _():
            stage_c(i - 2)

    loop(chunks + 2, step)

    def drain_send(i):
        r, b = chunk_of(i)

        @pl.when(has_right & (r <= s))
        def _():
            g_copy(r, b, 1).wait_send()

        @pl.when(has_left & (r >= s))
        def _():
            g_copy(r, b, 0).wait_send()

        a_copy(i).wait_send()
        for k in range(1, nx):
            b_copy(i, k).wait_send()

        @pl.when(jnp.logical_not((r == s) & (home == t)))
        def _():
            f_copy(i, r, b).wait_send()

    loop(chunks, drain_send)

    def drain_prompt(r):
        @pl.when(has_right & (r <= s))
        def _():
            p_copy(r, 1).wait_send()

        @pl.when(has_left & (r >= s))
        def _():
            p_copy(r, 0).wait_send()

    loop(nseq, drain_prompt)

    def drain_out(m):
        b = lax.div(m, per * ntp)
        j = lax.div(lax.rem(m, per * ntp), ntp)
        u = lax.rem(m, ntp)

        @pl.when(jnp.logical_not((t * per + j == s) & (u == t)))
        def _():
            row = b * BLOCK + lax.rem(u, 2) * half + lax.div(u, 2) * quart
            pltpu.make_async_remote_copy(
                src_ref=final.at[0],
                dst_ref=out_ref.at[j, pl.ds(row, quart)],
                send_sem=f_send.at[0],
                recv_sem=f_recv.at[b, j, u],
                device_id={"seq": s, "tp": partner},
                device_id_type=MESH,
            ).wait_recv()

    loop(MAXB * per * ntp, drain_out)


def per_device(
    resp_queries, resp_keys, resp_values, prompt_keys, prompt_values, out_weight, resp_blocks
):
    nseq = lax.axis_size("seq")
    ntp = lax.axis_size("tp")
    rows, depth = resp_queries.shape
    assert rows == MAXB * BLOCK and nseq % ntp == 0 and ntp % 2 == 0
    nx, per, chunks = ntp // 2, nseq // ntp, nseq * MAXB
    cols = out_weight.shape[1]
    pkv = jnp.concatenate([prompt_keys, prompt_values], axis=1)
    quart = BLOCK // ntp
    bf = jnp.bfloat16
    dma = pltpu.SemaphoreType.DMA
    vmem = pl.BlockSpec(memory_space=pltpu.VMEM)
    out = pl.pallas_call(
        functools.partial(fused_kernel, nseq, ntp, depth // resp_keys.shape[1]),
        out_shape=jax.ShapeDtypeStruct((per, rows, cols), bf),
        in_specs=[pl.BlockSpec(memory_space=pltpu.SMEM)] + [vmem] * 5,
        out_specs=vmem,
        scratch_shapes=[
            pltpu.VMEM((nseq * pkv.shape[0], pkv.shape[1]), bf),
            pltpu.VMEM((nseq, MAXB, BLOCK, depth), bf),
            pltpu.VMEM((chunks, BLOCK, cols), bf),
            pltpu.VMEM((chunks, BLOCK // 2, cols), bf),
            pltpu.VMEM((chunks, max(nx - 1, 1), quart, cols), bf),
            pltpu.VMEM((chunks, quart, cols), bf),
            dma((2, nseq)),
            dma((nseq,)),
            dma((2, nseq, MAXB)),
            dma((nseq, MAXB)),
            dma((chunks,)),
            dma((chunks,)),
            dma((chunks, max(nx - 1, 1))),
            dma((chunks, max(nx - 1, 1))),
            dma((chunks,)),
            dma((MAXB, per, ntp)),
        ],
        compiler_params=pltpu.CompilerParams(
            has_side_effects=True, vmem_limit_bytes=61000 * 1024
        ),
    )(resp_blocks, resp_queries, resp_keys, resp_values, pkv, out_weight)
    return out.transpose(1, 0, 2).reshape(rows, per * cols)


def solution(mesh):
    return jax.shard_map(
        per_device,
        mesh=mesh,
        in_specs=(
            P(("groups", "seq"), "tp"),
            P(("groups", "seq"), "tp"),
            P(("groups", "seq"), "tp"),
            P(("groups", "seq"), "tp"),
            P(("groups", "seq"), "tp"),
            P("tp", "seq"),
            P("groups"),
        ),
        out_specs=P(("groups", "seq"), "tp"),
        check_vma=False,
    )
```
